32 devices in a mesh: grp: 4 (over x, core), blk: 8 (over z, y).
Axes of the slice: x: 2, y: 2, z: 4, core: 2. Of those that a mesh axis runs over, the one named last changes fastest.
Arguments:
- orbitals: bfloat16 [8192, 4096], P(('blk', 'grp')), may hold values from -0.75 to 0.75
- point_cells: int32 [512], P(('grp', 'blk')), may hold values from 0 to 255
- point_count: int32 [32], P(('grp', 'blk')), may hold values from 1 to 16
Outputs:
- numerators: bfloat16 [8192, 512], P('blk', 'grp')
- gram: float32 [4, 128, 512], P(None, 'blk', 'grp')
The draws below stay inside these ranges and needn't reach their ends.
Inputs may be any that keep to these rules, and one draw needn't show every extreme that they name: Slots from point_count[d] on of owner d are empty and give zero columns; no slot of an owner past its count is read as live.
All inputs are finite; a program needn't handle non-finite values.
Results may differ from the reference program's by a relative error of at most 0.001.
Values may be sent and summed in bfloat16 or wider, within the bound.
A program may use at most 128 MiB of HBM per device.

```python
import jax
import jax.numpy as jnp
from jax import lax

ORB = 4096
CELLS_DEV = 256
CAP = 16
GRID = 8192
NPTS = 512
N_GRP = 4
N_BLK = 8


def with_ends(result, rng, low, high):
    dims = result.shape
    place = [jax.random.randint(jax.random.fold_in(rng, axis), (), 0, dims[axis]) for axis in range(len(dims))]
    result = result.at[tuple(place)].set(low)
    longest = dims.index(max(dims))
    place[longest] = (place[longest] + 1) % dims[longest]
    return result.at[tuple(place)].set(high)


def shard_levels(stream_key, dims, cuts, smallest, high):
    factor_of = 1.0
    for position, blocks in cuts:
        draws = jax.random.uniform(jax.random.fold_in(jax.random.fold_in(stream_key, 6), position), (blocks,), jnp.float32, smallest / len(cuts), high / len(cuts))
        factor_of = factor_of * jnp.repeat(jnp.exp(draws), dims[position] // blocks).reshape((-1,) + (1,) * (len(dims) - 1 - position))
    return factor_of


def gaussian(key, dims, scale, most, split=(), kind=jnp.bfloat16):
    entries = jax.random.normal(key, dims, jnp.float32) * scale
    if len(split) > 0:
        entries = shard_levels(key, dims, split, -0.22, 0.18) * entries
    return jnp.clip(entries, min=-most, max=most).astype(kind)


def setup_inputs(seed: int = 0) -> dict:
    streams_of = jax.random.split(jax.random.key(seed), 4)
    orbitals = gaussian(streams_of[0], (GRID, ORB), 0.125, 0.75, ((0, 32),))
    point_cells = with_ends(jax.random.randint(streams_of[1], (NPTS,), 0, CELLS_DEV), jax.random.fold_in(streams_of[1], 1), 0, CELLS_DEV - 1).astype(jnp.int32)
    point_count = with_ends(jax.random.randint(streams_of[2], (N_GRP * N_BLK,), 1, CAP + 1), jax.random.fold_in(streams_of[2], 1), 1, CAP).astype(jnp.int32)
    return dict(orbitals=orbitals, point_cells=point_cells, point_count=point_count)


def reference(orbitals, point_cells, point_count):
    slot_index = jnp.arange(NPTS, dtype=jnp.int32)
    owner_index = slot_index // CAP
    slot_within = slot_index % CAP
    group_index = owner_index // N_BLK
    block_index = owner_index % N_BLK
    row_block = block_index * N_GRP + group_index
    global_cells = (row_block * CELLS_DEV + point_cells).astype(jnp.int32)
    slot_live = (slot_within < jnp.take(point_count, owner_index)).astype(orbitals.dtype)
    points = jnp.take(orbitals, global_cells, axis=0) * slot_live[:, None]

    def slab_numerators(slab_rows):
        product = lax.dot_general(slab_rows, points, (((1,), (1,)), ((), ())), preferred_element_type=jnp.float32)
        return (product * product).astype(jnp.bfloat16)

    slabs = orbitals.reshape(N_BLK, CELLS_DEV * N_GRP, ORB)
    numerators = lax.map(slab_numerators, slabs).reshape(GRID, NPTS)
    product = lax.dot_general(points, points, (((1,), (1,)), ((), ())), preferred_element_type=jnp.float32)
    gram = (product * product).reshape(N_GRP, NPTS // N_GRP, NPTS)
    return numerators, gram
```

```python
import jax
import jax.numpy as jnp
from jax import lax
from jax.sharding import PartitionSpec as P


def pair_square(left, right):
    product = lax.dot_general(
        left, right, (((1,), (1,)), ((), ())), preferred_element_type=jnp.float32
    )
    return product * product


def per_device(orbitals, point_cells, point_count):
    cells, width = orbitals.shape
    capacity = point_cells.shape[0]
    groups = lax.axis_size("grp")
    blocks = lax.axis_size("blk")
    quarter_len = capacity * blocks
    slot_live = (jnp.arange(capacity, dtype=jnp.int32) < point_count[0]).astype(orbitals.dtype)
    own_points = jnp.take(orbitals, point_cells, axis=0) * slot_live[:, None]
    points = lax.all_gather(own_points, ("grp", "blk"), axis=0, tiled=True)
    mine = pair_square(orbitals, points).astype(jnp.bfloat16)
    mine = mine.reshape(cells, groups, quarter_len).transpose(1, 0, 2)
    numerators = lax.all_to_all(mine, "grp", 0, 0, tiled=True).reshape(groups * cells, quarter_len)
    by_owner = points.reshape(groups, blocks, capacity, width)
    across = lax.dynamic_index_in_dim(by_owner, lax.axis_index("blk"), 1, keepdims=False)
    quarter = lax.dynamic_index_in_dim(by_owner, lax.axis_index("grp"), 0, keepdims=False)
    gram = pair_square(
        across.reshape(groups * capacity, width), quarter.reshape(quarter_len, width)
    ).reshape(groups, capacity, quarter_len)
    return (numerators, gram)


def solution(mesh):
    in_specs = (P(("blk", "grp"), None), P(("grp", "blk")), P(("grp", "blk")))
    out_specs = (P("blk", "grp"), P(None, "blk", "grp"))
    return jax.shard_map(
        per_device, mesh=mesh, in_specs=in_specs, out_specs=out_specs, check_vma=False
    )
```

```python
import functools

import jax
import jax.numpy as jnp
from jax import lax
from jax.experimental import pallas as pl
from jax.experimental.pallas import tpu as pltpu
from jax.sharding import PartitionSpec as P

MESH = pl.DeviceIdType.MESH
ORDERS = ("xzy", "yzx", "zxy", "zyx")
CHUNKS = len(ORDERS)
LONGEST_LINE = 4


def dot_nt(left, right):
    return lax.dot_general(
        left, right, (((1,), (1,)), ((), ())), preferred_element_type=jnp.float32
    )


def pair_square(left, right):
    product = dot_nt(left, right)
    return product * product


def per_device(orbitals, point_cells, point_count):
    cells, width = orbitals.shape
    capacity = point_cells.shape[0]
    groups = lax.axis_size("grp")
    blocks = lax.axis_size("blk")
    quarter_len = capacity * blocks
    slot_live = (jnp.arange(capacity, dtype=jnp.int32) < point_count[0]).astype(orbitals.dtype)
    own_points = jnp.take(orbitals, point_cells, axis=0) * slot_live[:, None]
    points = lax.all_gather(own_points, ("grp", "blk"), axis=0, tiled=True)
    mine = pair_square(orbitals, points).astype(jnp.bfloat16)
    mine = mine.reshape(cells, groups, quarter_len).transpose(1, 0, 2)
    numerators = lax.all_to_all(mine, "grp", 0, 0, tiled=True).reshape(groups * cells, quarter_len)
    by_owner = points.reshape(groups, blocks, capacity, width)
    across = lax.dynamic_index_in_dim(by_owner, lax.axis_index("blk"), 1, keepdims=False)
    quarter = lax.dynamic_index_in_dim(by_owner, lax.axis_index("grp"), 0, keepdims=False)
    gram = pair_square(
        across.reshape(groups * capacity, width), quarter.reshape(quarter_len, width)
    ).reshape(groups, capacity, quarter_len)
    return (numerators, gram)


def kernel(groups, blocks, capacity, cells_ref, count_ref, orb_hbm, num_ref, gram_ref,
           orb, pts, res, orb_sem, own_sem, recv, precv, zsend, xsend, ysend, psend, rsend, rrecv):
    g = lax.axis_index("grp")
    b = lax.axis_index("blk")
    line = blocks // 2
    x, c = g // 2, g % 2
    z, y = b // 2, b % 2
    rows, width = orb.shape
    part = width // CHUNKS
    other_core = x * 2 + 1 - c
    other_x = (1 - x) * 2 + c
    far_core = (1 - x) * 2 + 1 - c
    other_y = z * 2 + 1 - y
    quarter_len = capacity * blocks

    load = pltpu.make_async_copy(orb_hbm, orb, orb_sem)
    load.start()

    barrier = pltpu.get_barrier_semaphore()

    def greet(gg, bb):
        pl.semaphore_signal(barrier, inc=1, device_id={"grp": gg, "blk": bb}, device_id_type=MESH)

    greet(other_core, b)
    greet(other_x, b)
    greet(far_core, b)
    greet(g, other_y)

    @pl.when(z > 0)
    def _():
        greet(g, b - 2)

    @pl.when(z < line - 1)
    def _():
        greet(g, b + 2)

    load.wait()
    slot = lax.broadcasted_iota(jnp.int32, (capacity, rows), 0)
    cell = lax.broadcasted_iota(jnp.int32, (capacity, rows), 1)
    wanted = jnp.full((capacity, rows), -1, jnp.int32)
    for j in range(capacity):
        wanted = jnp.where(slot == j, cells_ref[j], wanted)
    wanted = jnp.where(slot < count_ref[0], wanted, -1)
    pick = jnp.where(cell == wanted, 1.0, 0.0).astype(jnp.bfloat16)
    own_rows = pl.ds(pl.multiple_of((g * blocks + b) * capacity, capacity), capacity)
    pts[own_rows, :] = jnp.dot(pick, orb[...], preferred_element_type=jnp.float32).astype(jnp.bfloat16)

    inner = (z > 0) & (z < line - 1)

    @pl.when(inner)
    def _():
        pl.semaphore_wait(barrier, 6)

    @pl.when(jnp.logical_not(inner))
    def _():
        pl.semaphore_wait(barrier, 5)

    def piece(q, core, sz, k):
        xx = 1 - x if q in (1, 3) else x
        yy = 1 - y if q in (2, 3) else y
        owner = (xx * 2 + core) * blocks + sz * 2 + yy
        return pts.at[pl.ds(pl.multiple_of(owner * capacity, capacity), capacity),
                      pl.ds(k * part, part)]

    def move(q, sz, k, send_sem, recv_sem, gg, bb):
        ref = piece(q, c, sz, k)
        return pltpu.make_async_remote_copy(
            src_ref=ref, dst_ref=ref, send_sem=send_sem, recv_sem=recv_sem,
            device_id={"grp": gg, "blk": bb}, device_id_type=MESH)

    def along_z(q, sz, k, way):
        return move(q, sz, k, zsend.at[(way + 1) // 2, (q + 1) // 2, sz, k], recv.at[q, sz, k],
                    g, b + 2 * way)

    def over_x(q, sz, k):
        return move(q, sz, k, xsend.at[q // 2, sz, k], recv.at[q + 1, sz, k], other_x, b)

    def over_y(q, sz, k):
        return move(q, sz, k, ysend.at[q, sz, k], recv.at[q + 2, sz, k], g, other_y)

    def to_core(q, sz, k):
        return move(q, sz, k, psend.at[q, sz, k], precv.at[q, sz, k], other_core, b)

    def arrived(q, sz, k):
        ref = piece(q, c, sz, k)
        pltpu.make_async_copy(ref, ref, recv.at[q, sz, k]).wait()

    def core_arrived(q, sz, k):
        ref = piece(q, 1 - c, sz, k)
        pltpu.make_async_copy(ref, ref, precv.at[q, sz, k]).wait()

    def sends(q, sz, k, sign, act):
        done = {0: "", 1: "x", 2: "y", 3: "xy"}[q] + ("z" if sign != 0 else "")
        reached = max([ORDERS[k].index(d) for d in done], default=-1)
        later = ORDERS[k][reached + 1:]
        down_too = ("z" in later) or (done != "" and ORDERS[k][reached] == "z" and sign > 0)
        up_too = ("z" in later) or (done != "" and ORDERS[k][reached] == "z" and sign < 0)
        if down_too:
            @pl.when(z > 0)
            def _():
                act(along_z(q, sz, k, -1))
        if up_too:
            @pl.when(z < line - 1)
            def _():
                act(along_z(q, sz, k, 1))
        if "x" in later:
            act(over_x(q, sz, k))
        if "y" in later:
            act(over_y(q, sz, k))
        act(to_core(q, sz, k))

    def take(q, sz, k, sign):
        if q != 0 or sign != 0:
            arrived(q, sz, k)
        sends(q, sz, k, sign, lambda copy: copy.start())

    def sent(q, sz, k, sign):
        sends(q, sz, k, sign, lambda copy: copy.wait_send())

    def walk(act, wave):
        for stage, quadrants in enumerate(((0,), (1, 2), (3,))):
            s = wave - stage
            if s < 0 or s > line - 1:
                continue
            for k in range(CHUNKS):
                for sign in ((0,) if s == 0 else (1, -1)):
                    sz = z + sign * s

                    def both(sz=sz, k=k, sign=sign):
                        for q in quadrants:
                            act(q, sz, k, sign)

                    if sign == 0:
                        both()
                    elif sign > 0:
                        pl.when(z + s < line)(both)
                    else:
                        pl.when(z - s >= 0)(both)

    def squares(xx):
        points = pts[pl.ds(pl.multiple_of(xx * 2 * quarter_len, capacity), 2 * quarter_len), :]
        return pair_square(orb[...], points).astype(jnp.bfloat16)

    def result_copy(i, gg):
        return pltpu.make_async_remote_copy(
            src_ref=res.at[i],
            dst_ref=num_ref.at[pl.ds(pl.multiple_of(g * rows, rows), rows), :],
            send_sem=rsend.at[i], recv_sem=rrecv.at[i],
            device_id={"grp": gg, "blk": b}, device_id_type=MESH)

    def own_result():
        return pltpu.make_async_copy(
            res.at[0], num_ref.at[pl.ds(pl.multiple_of(g * rows, rows), rows), :], own_sem)

    for wave in range(line + 2):
        walk(take, wave)
        if wave == line:
            for q in (0, 2, 1):
                for sz in range(line):
                    for k in range(CHUNKS):
                        core_arrived(q, sz, k)
            near = squares(x)
            first = near[:, :quarter_len]
            second = near[:, quarter_len:]
            res[0] = jnp.where(c == 0, first, second)
            res[1] = jnp.where(c == 0, second, first)
            quarter = pts[pl.ds(pl.multiple_of(g * quarter_len, quarter_len), quarter_len), :]
            across = jnp.concatenate(
                [pts[pl.ds(pl.multiple_of((a * blocks + b) * capacity, capacity), capacity), :]
                 for a in range(groups)], axis=0)
            gram_ref[...] = pair_square(across, quarter).reshape(groups, capacity, quarter_len)
            own_result().start()
            result_copy(1, other_core).start()

    for sz in range(line):
        for k in range(CHUNKS):
            core_arrived(3, sz, k)
    far = squares(1 - x)
    first = far[:, :quarter_len]
    second = far[:, quarter_len:]
    res[2] = jnp.where(c == 0, first, second)
    res[3] = jnp.where(c == 0, second, first)
    result_copy(2, other_x).start()
    result_copy(3, far_core).start()

    for wave in range(line + 2):
        walk(sent, wave)
    own_result().wait()
    for i, gg in ((1, other_core), (2, other_x), (3, far_core)):
        result_copy(i, gg).wait_send()
        spot = num_ref.at[pl.ds(pl.multiple_of(gg * rows, rows), rows), :]
        pltpu.make_async_copy(spot, spot, rrecv.at[i]).wait()


def per_device_kernel(orbitals, point_cells, point_count):
    cells, width = orbitals.shape
    capacity = point_cells.shape[0]
    groups = lax.axis_size("grp")
    blocks = lax.axis_size("blk")
    line = blocks // 2
    quarter_len = capacity * blocks
    dma = pltpu.SemaphoreType.DMA
    return pl.pallas_call(
        functools.partial(kernel, groups, blocks, capacity),
        out_shape=(
            jax.ShapeDtypeStruct((groups * cells, quarter_len), jnp.bfloat16),
            jax.ShapeDtypeStruct((groups, capacity, quarter_len), jnp.float32),
        ),
        in_specs=[
            pl.BlockSpec(memory_space=pltpu.SMEM),
            pl.BlockSpec(memory_space=pltpu.SMEM),
            pl.BlockSpec(memory_space=pltpu.HBM),
        ],
        out_specs=(
            pl.BlockSpec(memory_space=pl.ANY),
            pl.BlockSpec(memory_space=pltpu.VMEM),
        ),
        scratch_shapes=[
            pltpu.VMEM((cells, width), jnp.bfloat16),
            pltpu.VMEM((groups * quarter_len, width), jnp.bfloat16),
            pltpu.VMEM((groups, cells, quarter_len), jnp.bfloat16),
            dma, dma,
            dma((4, line, CHUNKS)), dma((4, line, CHUNKS)),
            dma((2, 2, line, CHUNKS)), dma((2, line, CHUNKS)), dma((2, line, CHUNKS)),
            dma((4, line, CHUNKS)),
            dma((groups,)), dma((groups,)),
        ],
        compiler_params=pltpu.CompilerParams(
            collective_id=0, has_side_effects=True, vmem_limit_bytes=62 * 1024 * 1024 + 512 * 1024
        ),
    )(point_cells, point_count, orbitals)


def solution(mesh):
    in_specs = (P(("blk", "grp"), None), P(("grp", "blk")), P(("grp", "blk")))
    out_specs = (P("blk", "grp"), P(None, "blk", "grp"))
    groups, blocks = mesh.shape["grp"], mesh.shape["blk"]
    fits = groups == 4 and blocks % 2 == 0 and 2 <= blocks // 2 <= LONGEST_LINE
    return jax.shard_map(
        per_device_kernel if fits else per_device,
        mesh=mesh, in_specs=in_specs, out_specs=out_specs, check_vma=False
    )
```

```python
import functools

import jax
import jax.numpy as jnp
from jax import lax
from jax.experimental import pallas as pl
from jax.experimental.pallas import tpu as pltpu
from jax.sharding import PartitionSpec as P

MESH = pl.DeviceIdType.MESH
ORDERS = ("zxy", "zyx")
CHUNKS = len(ORDERS)
LONGEST_LINE = 4


def dot_nt(left, right):
    return lax.dot_general(
        left, right, (((1,), (1,)), ((), ())), preferred_element_type=jnp.float32
    )


def pair_square(left, right):
    product = dot_nt(left, right)
    return product * product


def per_device(orbitals, point_cells, point_count):
    cells, width = orbitals.shape
    capacity = point_cells.shape[0]
    groups = lax.axis_size("grp")
    blocks = lax.axis_size("blk")
    quarter_len = capacity * blocks
    slot_live = (jnp.arange(capacity, dtype=jnp.int32) < point_count[0]).astype(orbitals.dtype)
    own_points = jnp.take(orbitals, point_cells, axis=0) * slot_live[:, None]
    points = lax.all_gather(own_points, ("grp", "blk"), axis=0, tiled=True)
    mine = pair_square(orbitals, points).astype(jnp.bfloat16)
    mine = mine.reshape(cells, groups, quarter_len).transpose(1, 0, 2)
    numerators = lax.all_to_all(mine, "grp", 0, 0, tiled=True).reshape(groups * cells, quarter_len)
    by_owner = points.reshape(groups, blocks, capacity, width)
    across = lax.dynamic_index_in_dim(by_owner, lax.axis_index("blk"), 1, keepdims=False)
    quarter = lax.dynamic_index_in_dim(by_owner, lax.axis_index("grp"), 0, keepdims=False)
    gram = pair_square(
        across.reshape(groups * capacity, width), quarter.reshape(quarter_len, width)
    ).reshape(groups, capacity, quarter_len)
    return (numerators, gram)


def kernel(groups, blocks, capacity, cells_ref, count_ref, orb, num_ref, gram_ref,
           pts, res, own_sem, recv, precv, zsend, xsend, ysend, psend, rsend, rrecv):
    g = lax.axis_index("grp")
    b = lax.axis_index("blk")
    line = blocks // 2
    x, c = g // 2, g % 2
    z, y = b // 2, b % 2
    rows, width = orb.shape
    part = width // CHUNKS
    other_core = x * 2 + 1 - c
    other_x = (1 - x) * 2 + c
    far_core = (1 - x) * 2 + 1 - c
    other_y = z * 2 + 1 - y
    quarter_len = capacity * blocks

    barrier = pltpu.get_barrier_semaphore()

    def greet(gg, bb):
        pl.semaphore_signal(barrier, inc=1, device_id={"grp": gg, "blk": bb}, device_id_type=MESH)

    greet(other_core, b)
    greet(other_x, b)
    greet(far_core, b)
    greet(g, other_y)

    @pl.when(z > 0)
    def _():
        greet(g, b - 2)

    @pl.when(z < line - 1)
    def _():
        greet(g, b + 2)

    slot = lax.broadcasted_iota(jnp.int32, (capacity, rows), 0)
    cell = lax.broadcasted_iota(jnp.int32, (capacity, rows), 1)
    wanted = jnp.full((capacity, rows), -1, jnp.int32)
    for j in range(capacity):
        wanted = jnp.where(slot == j, cells_ref[j], wanted)
    wanted = jnp.where(slot < count_ref[0], wanted, -1)
    pick = jnp.where(cell == wanted, 1.0, 0.0).astype(jnp.bfloat16)
    own_rows = pl.ds(pl.multiple_of((g * blocks + b) * capacity, capacity), capacity)
    pts[own_rows, :] = jnp.dot(pick, orb[...], preferred_element_type=jnp.float32).astype(jnp.bfloat16)

    inner = (z > 0) & (z < line - 1)

    @pl.when(inner)
    def _():
        pl.semaphore_wait(barrier, 6)

    @pl.when(jnp.logical_not(inner))
    def _():
        pl.semaphore_wait(barrier, 5)

    def piece(q, core, sz, k):
        xx = 1 - x if q in (1, 3) else x
        yy = 1 - y if q in (2, 3) else y
        owner = (xx * 2 + core) * blocks + sz * 2 + yy
        return pts.at[pl.ds(pl.multiple_of(owner * capacity, capacity), capacity),
                      pl.ds(k * part, part)]

    def move(q, sz, k, send_sem, recv_sem, gg, bb):
        ref = piece(q, c, sz, k)
        return pltpu.make_async_remote_copy(
            src_ref=ref, dst_ref=ref, send_sem=send_sem, recv_sem=recv_sem,
            device_id={"grp": gg, "blk": bb}, device_id_type=MESH)

    def along_z(q, sz, k, way):
        return move(q, sz, k, zsend.at[(way + 1) // 2, (q + 1) // 2, sz, k], recv.at[q, sz, k],
                    g, b + 2 * way)

    def over_x(q, sz, k):
        return move(q, sz, k, xsend.at[q // 2, sz, k], recv.at[q + 1, sz, k], other_x, b)

    def over_y(q, sz, k):
        return move(q, sz, k, ysend.at[q, sz, k], recv.at[q + 2, sz, k], g, other_y)

    def to_core(q, sz, k):
        return move(q, sz, k, psend.at[q, sz, k], precv.at[q, sz, k], other_core, b)

    def arrived(q, sz, k):
        ref = piece(q, c, sz, k)
        pltpu.make_async_copy(ref, ref, recv.at[q, sz, k]).wait()

    def core_arrived(q, sz, k):
        ref = piece(q, 1 - c, sz, k)
        pltpu.make_async_copy(ref, ref, precv.at[q, sz, k]).wait()

    def sends(q, sz, k, sign, act):
        done = {0: "", 1: "x", 2: "y", 3: "xy"}[q] + ("z" if sign != 0 else "")
        reached = max([ORDERS[k].index(d) for d in done], default=-1)
        later = ORDERS[k][reached + 1:]
        down_too = ("z" in later) or (done != "" and ORDERS[k][reached] == "z" and sign > 0)
        up_too = ("z" in later) or (done != "" and ORDERS[k][reached] == "z" and sign < 0)
        if down_too:
            @pl.when(z > 0)
            def _():
                act(along_z(q, sz, k, -1))
        if up_too:
            @pl.when(z < line - 1)
            def _():
                act(along_z(q, sz, k, 1))
        if "x" in later:
            act(over_x(q, sz, k))
        if "y" in later:
            act(over_y(q, sz, k))
        act(to_core(q, sz, k))

    def take(q, sz, k, sign):
        if q != 0 or sign != 0:
            arrived(q, sz, k)
        sends(q, sz, k, sign, lambda copy: copy.start())

    def sent(q, sz, k, sign):
        sends(q, sz, k, sign, lambda copy: copy.wait_send())

    def walk(act, wave):
        for stage, quadrants in enumerate(((0,), (1, 2), (3,))):
            s = wave - stage
            if s < 0 or s > line - 1:
                continue
            for k in range(CHUNKS):
                for sign in ((0,) if s == 0 else (1, -1)):
                    sz = z + sign * s

                    def both(sz=sz, k=k, sign=sign):
                        for q in quadrants:
                            act(q, sz, k, sign)

                    if sign == 0:
                        both()
                    elif sign > 0:
                        pl.when(z + s < line)(both)
                    else:
                        pl.when(z - s >= 0)(both)

    def squares(xx):
        points = pts[pl.ds(pl.multiple_of(xx * 2 * quarter_len, capacity), 2 * quarter_len), :]
        return pair_square(orb[...], points).astype(jnp.bfloat16)

    def result_copy(i, gg):
        return pltpu.make_async_remote_copy(
            src_ref=res.at[i],
            dst_ref=num_ref.at[pl.ds(pl.multiple_of(g * rows, rows), rows), :],
            send_sem=rsend.at[i], recv_sem=rrecv.at[i],
            device_id={"grp": gg, "blk": b}, device_id_type=MESH)

    def own_result():
        return pltpu.make_async_copy(
            res.at[0], num_ref.at[pl.ds(pl.multiple_of(g * rows, rows), rows), :], own_sem)

    for wave in range(line + 2):
        walk(take, wave)
        if wave == line:
            for q in (0, 2, 1):
                for sz in range(line):
                    for k in range(CHUNKS):
                        core_arrived(q, sz, k)
            near = squares(x)
            first = near[:, :quarter_len]
            second = near[:, quarter_len:]
            res[0] = jnp.where(c == 0, first, second)
            res[1] = jnp.where(c == 0, second, first)
            quarter = pts[pl.ds(pl.multiple_of(g * quarter_len, quarter_len), quarter_len), :]
            across = jnp.concatenate(
                [pts[pl.ds(pl.multiple_of((a * blocks + b) * capacity, capacity), capacity), :]
                 for a in range(groups)], axis=0)
            gram_ref[...] = pair_square(across, quarter).reshape(groups, capacity, quarter_len)
            own_result().start()
            result_copy(1, other_core).start()

    for sz in range(line):
        for k in range(CHUNKS):
            core_arrived(3, sz, k)
    far = squares(1 - x)
    first = far[:, :quarter_len]
    second = far[:, quarter_len:]
    res[2] = jnp.where(c == 0, first, second)
    res[3] = jnp.where(c == 0, second, first)
    result_copy(2, other_x).start()
    result_copy(3, far_core).start()

    for wave in range(line + 2):
        walk(sent, wave)
    own_result().wait()
    for i, gg in ((1, other_core), (2, other_x), (3, far_core)):
        result_copy(i, gg).wait_send()
        spot = num_ref.at[pl.ds(pl.multiple_of(gg * rows, rows), rows), :]
        pltpu.make_async_copy(spot, spot, rrecv.at[i]).wait()


def per_device_kernel(orbitals, point_cells, point_count):
    cells, width = orbitals.shape
    capacity = point_cells.shape[0]
    groups = lax.axis_size("grp")
    blocks = lax.axis_size("blk")
    line = blocks // 2
    quarter_len = capacity * blocks
    dma = pltpu.SemaphoreType.DMA
    return pl.pallas_call(
        functools.partial(kernel, groups, blocks, capacity),
        out_shape=(
            jax.ShapeDtypeStruct((groups * cells, quarter_len), jnp.bfloat16),
            jax.ShapeDtypeStruct((groups, capacity, quarter_len), jnp.float32),
        ),
        in_specs=[
            pl.BlockSpec(memory_space=pltpu.SMEM),
            pl.BlockSpec(memory_space=pltpu.SMEM),
            pl.BlockSpec(memory_space=pltpu.VMEM),
        ],
        out_specs=(
            pl.BlockSpec(memory_space=pl.ANY),
            pl.BlockSpec(memory_space=pltpu.VMEM),
        ),
        scratch_shapes=[
            pltpu.VMEM((groups * quarter_len, width), jnp.bfloat16),
            pltpu.VMEM((groups, cells, quarter_len), jnp.bfloat16),
            dma,
            dma((4, line, CHUNKS)), dma((4, line, CHUNKS)),
            dma((2, 2, line, CHUNKS)), dma((2, line, CHUNKS)), dma((2, line, CHUNKS)),
            dma((4, line, CHUNKS)),
            dma((groups,)), dma((groups,)),
        ],
        compiler_params=pltpu.CompilerParams(
            collective_id=0, has_side_effects=True, vmem_limit_bytes=48 * 1024 * 1024
        ),
    )(point_cells, point_count, orbitals)


def solution(mesh):
    in_specs = (P(("blk", "grp"), None), P(("grp", "blk")), P(("grp", "blk")))
    out_specs = (P("blk", "grp"), P(None, "blk", "grp"))
    groups, blocks = mesh.shape["grp"], mesh.shape["blk"]
    fits = groups == 4 and blocks % 2 == 0 and 2 <= blocks // 2 <= LONGEST_LINE
    return jax.shard_map(
        per_device_kernel if fits else per_device,
        mesh=mesh, in_specs=in_specs, out_specs=out_specs, check_vma=False
    )
```
